8 devices in a mesh: pod: 2 (over z, y), data: 4 (over x, core).
Axes of the slice: x: 2, y: 2, z: 1, core: 2. Of those that a mesh axis runs over, the one named last changes fastest.
Arguments:
- feat_a: bfloat16 [8192, 2048], P(('pod', 'data'))
- feat_b: bfloat16 [8192, 2048], P(('pod', 'data'))
- w_first: bfloat16 [2048, 2048], replicated
- w_second: bfloat16 [2048, 2048], replicated
- w_third: bfloat16 [2048, 2048], replicated
- gain_first: float32 [2048], replicated
- shift_first: float32 [2048], replicated
- gain_second: float32 [2048], replicated
- shift_second: float32 [2048], replicated
- lam_off: float32 [], replicated
Outputs:
- output 1: float32 [], replicated
- output 2: float32 [2048, 2048], replicated
- output 3: float32 [2048, 2048], replicated
- output 4: float32 [2048, 2048], replicated
- output 5: float32 [2048], replicated
- output 6: float32 [2048], replicated
- output 7: float32 [2048], replicated
- output 8: float32 [2048], replicated
All inputs are finite; a program needn't handle non-finite values.
Results may differ from the reference program's by a relative error of at most 0.001.
Values are sent between devices in bfloat16 or wider.
A program may use at most 1 GiB of HBM per device.

```python
import jax
import jax.numpy as jnp
from jax import lax

ROWS_DEV = 1024
NUM_DEVICES = 8
FEAT_DIM = 2048
PROJ_DIM = 2048
NUM_ROWS = ROWS_DEV * NUM_DEVICES
BN_EPS = 1e-5


def setup_inputs(seed: int = 0) -> dict:
    key_list = jax.random.split(jax.random.key(seed), 12)
    block_shape = (NUM_DEVICES, ROWS_DEV, FEAT_DIM)
    stat_shape = (NUM_DEVICES, 1, FEAT_DIM)
    base_vals = jax.random.normal(key_list[0], block_shape, jnp.float32)
    noise_vals = jax.random.normal(key_list[1], block_shape, jnp.float32)
    shard_shift = 0.7 * jax.random.normal(key_list[2], stat_shape, jnp.float32)
    shard_scale = jax.random.uniform(key_list[3], stat_shape, jnp.float32, 0.5, 1.5)
    view_a = base_vals * shard_scale + shard_shift
    view_b = (0.8 * base_vals + 0.6 * noise_vals) * shard_scale + shard_shift
    w_first = jax.random.normal(key_list[4], (FEAT_DIM, PROJ_DIM), jnp.float32) * FEAT_DIM ** -0.5
    w_second = jax.random.normal(key_list[5], (PROJ_DIM, PROJ_DIM), jnp.float32) * PROJ_DIM ** -0.5
    w_third = jax.random.normal(key_list[6], (PROJ_DIM, PROJ_DIM), jnp.float32) * PROJ_DIM ** -0.5
    lam_off = (0.05 + 0.1 * jax.random.uniform(key_list[11], (), jnp.float32)) * NUM_ROWS / PROJ_DIM
    return {
        'feat_a': view_a.reshape(NUM_ROWS, FEAT_DIM).astype(jnp.bfloat16),
        'feat_b': view_b.reshape(NUM_ROWS, FEAT_DIM).astype(jnp.bfloat16),
        'w_first': w_first.astype(jnp.bfloat16),
        'w_second': w_second.astype(jnp.bfloat16),
        'w_third': w_third.astype(jnp.bfloat16),
        'gain_first': 1.0 + 0.3 * jax.random.normal(key_list[7], (PROJ_DIM,), jnp.float32),
        'shift_first': 0.5 * jax.random.normal(key_list[8], (PROJ_DIM,), jnp.float32),
        'gain_second': 1.0 + 0.3 * jax.random.normal(key_list[9], (PROJ_DIM,), jnp.float32),
        'shift_second': 0.5 * jax.random.normal(key_list[10], (PROJ_DIM,), jnp.float32),
        'lam_off': lam_off,
    }


def batch_norm(pre_act):
    feat_mean = jnp.sum(pre_act, axis=0) / NUM_ROWS
    sq_mean = jnp.sum(pre_act * pre_act, axis=0) / NUM_ROWS
    inv_std = lax.rsqrt(sq_mean - feat_mean * feat_mean + BN_EPS)
    return (pre_act - feat_mean) * inv_std, inv_std


def project(feats_in, w_first, w_second, w_third, gain_first, shift_first, gain_second, shift_second):
    pre_one = jnp.dot(feats_in, w_first, preferred_element_type=jnp.float32)
    norm_one, inv_one = batch_norm(pre_one)
    post_one = gain_first * norm_one + shift_first
    hid_one = jnp.maximum(post_one, 0.0).astype(jnp.bfloat16)
    pre_two = jnp.dot(hid_one, w_second, preferred_element_type=jnp.float32)
    norm_two, inv_two = batch_norm(pre_two)
    post_two = gain_second * norm_two + shift_second
    hid_two = jnp.maximum(post_two, 0.0).astype(jnp.bfloat16)
    proj_out = jnp.dot(hid_two, w_third, preferred_element_type=jnp.float32)
    emb_norm, inv_three = batch_norm(proj_out)
    return (norm_one, inv_one, post_one, hid_one, norm_two, inv_two, post_two, hid_two, emb_norm, inv_three)


def norm_backward(grad_norm, normed, inv_std):
    grad_mean = jnp.sum(grad_norm, axis=0) / NUM_ROWS
    cross_mean = jnp.sum(grad_norm * normed, axis=0) / NUM_ROWS
    return inv_std * (grad_norm - grad_mean - normed * cross_mean)


def back_project(grad_emb, feats_in, saved, w_second, w_third, gain_first, gain_second):
    norm_one, inv_one, post_one, hid_one, norm_two, inv_two, post_two, hid_two, emb_norm, inv_three = saved
    grad_proj = norm_backward(grad_emb, emb_norm, inv_three).astype(jnp.bfloat16)
    grad_third = jnp.dot(hid_two.T, grad_proj, preferred_element_type=jnp.float32)
    grad_act_two = jnp.where(post_two > 0, jnp.dot(grad_proj, w_third.T, preferred_element_type=jnp.float32), 0.0)
    grad_gain_two = jnp.sum(grad_act_two * norm_two, axis=0)
    grad_shift_two = jnp.sum(grad_act_two, axis=0)
    grad_pre_two = norm_backward(gain_second * grad_act_two, norm_two, inv_two).astype(jnp.bfloat16)
    grad_second = jnp.dot(hid_one.T, grad_pre_two, preferred_element_type=jnp.float32)
    grad_act_one = jnp.where(post_one > 0, jnp.dot(grad_pre_two, w_second.T, preferred_element_type=jnp.float32), 0.0)
    grad_gain_one = jnp.sum(grad_act_one * norm_one, axis=0)
    grad_shift_one = jnp.sum(grad_act_one, axis=0)
    grad_pre_one = norm_backward(gain_first * grad_act_one, norm_one, inv_one).astype(jnp.bfloat16)
    grad_first = jnp.dot(feats_in.T, grad_pre_one, preferred_element_type=jnp.float32)
    return (grad_first, grad_second, grad_third, grad_gain_one, grad_shift_one, grad_gain_two, grad_shift_two)


def reference(feat_a, feat_b, w_first, w_second, w_third, gain_first, shift_first, gain_second, shift_second, lam_off):
    saved_a = project(feat_a, w_first, w_second, w_third, gain_first, shift_first, gain_second, shift_second)
    saved_b = project(feat_b, w_first, w_second, w_third, gain_first, shift_first, gain_second, shift_second)
    emb_a = saved_a[8].astype(jnp.bfloat16)
    emb_b = saved_b[8].astype(jnp.bfloat16)
    corr_mat = jnp.dot(emb_a.T, emb_b, preferred_element_type=jnp.float32) / NUM_ROWS
    on_diag = jnp.diagonal(corr_mat)
    total_loss = jnp.sum((1.0 - on_diag) ** 2) + lam_off * (jnp.sum(corr_mat * corr_mat) - jnp.sum(on_diag * on_diag))
    diag_mask = jnp.arange(PROJ_DIM)[:, None] == jnp.arange(PROJ_DIM)[None, :]
    grad_corr = jnp.where(diag_mask, -2.0 * (1.0 - corr_mat), 2.0 * lam_off * corr_mat).astype(jnp.bfloat16)
    grad_emb_a = jnp.dot(emb_b, grad_corr.T, preferred_element_type=jnp.float32) / NUM_ROWS
    grad_emb_b = jnp.dot(emb_a, grad_corr, preferred_element_type=jnp.float32) / NUM_ROWS
    grads_a = back_project(grad_emb_a, feat_a, saved_a, w_second, w_third, gain_first, gain_second)
    grads_b = back_project(grad_emb_b, feat_b, saved_b, w_second, w_third, gain_first, gain_second)
    return (total_loss, grads_a[0] + grads_b[0], grads_a[1] + grads_b[1], grads_a[2] + grads_b[2], grads_a[3] + grads_b[3], grads_a[4] + grads_b[4], grads_a[5] + grads_b[5], grads_a[6] + grads_b[6])
```

```python
import functools
import jax
import jax.numpy as jnp
from jax import lax
from jax.experimental import pallas as pl
from jax.experimental.pallas import tpu as pltpu
from jax.sharding import PartitionSpec as P

BN_EPS = 1e-5
ROW_AXES = ('pod', 'data')
NDEV = 8
BLK = 256


def exchange_kernel(in_ref, out_ref, slots, send_sems, recv_sems):
    pod = lax.axis_index('pod')
    data = lax.axis_index('data')
    me = pod * 4 + data
    barrier = pltpu.get_barrier_semaphore()
    for off in range(1, NDEV):
        peer = lax.rem(me + off, NDEV)
        pl.semaphore_signal(barrier, inc=1, device_id=(peer // 4, lax.rem(peer, 4)), device_id_type=pl.DeviceIdType.MESH)
    pl.semaphore_wait(barrier, NDEV - 1)
    copies = []
    for off in range(1, NDEV):
        peer = lax.rem(me + off, NDEV)
        copy = pltpu.make_async_remote_copy(
            src_ref=in_ref, dst_ref=slots.at[off], send_sem=send_sems.at[off], recv_sem=recv_sems.at[off],
            device_id=(peer // 4, lax.rem(peer, 4)), device_id_type=pl.DeviceIdType.MESH)
        copy.start()
        copies.append(copy)
    slots[0] = in_ref[...]
    for copy in copies:
        copy.wait()
    total = slots[me]
    for src in range(1, NDEV):
        total = total + slots[lax.rem(me + NDEV - src, NDEV)]
    out_ref[...] = total


def sum_devices(vals, cid):
    return pl.pallas_call(
        exchange_kernel,
        out_shape=jax.ShapeDtypeStruct(vals.shape, vals.dtype),
        in_specs=[pl.BlockSpec(memory_space=pltpu.VMEM)],
        out_specs=pl.BlockSpec(memory_space=pltpu.VMEM),
        scratch_shapes=[pltpu.VMEM((NDEV,) + vals.shape, vals.dtype), pltpu.SemaphoreType.DMA((NDEV,)), pltpu.SemaphoreType.DMA((NDEV,))],
        compiler_params=pltpu.CompilerParams(collective_id=cid, has_side_effects=True),
        name='stat_sum',
    )(vals)


CORE_PERM = [(d, d ^ 1) for d in range(8)]
FIRST_PERM = [(d, d ^ 2 if d % 2 == 0 else d ^ 4) for d in range(8)]
SECOND_PERM = [(d, d ^ 4 if d % 2 == 0 else d ^ 2) for d in range(8)]


def send(block, perm):
    return lax.ppermute(block, ROW_AXES, perm)


def place():
    y = lax.axis_index('pod')
    xc = lax.axis_index('data')
    core, x = lax.rem(xc, 2), xc // 2
    key1 = jnp.where(core == 0, x, y)
    key2 = jnp.where(core == 0, y, x)
    return core, key1, key2


def block_of(mat, idx):
    return lax.dynamic_slice_in_dim(mat, idx * BLK, BLK, axis=0)


def reduce_block(theirs, ours, where):
    core, key1, key2 = where
    got = send(theirs, CORE_PERM)
    b_sf, b_sk = (1 - key1) * 2 + 1 - key2, (1 - key1) * 2 + key2
    b_kf, b_kk = key1 * 2 + 1 - key2, key1 * 2 + key2
    in_f = send(block_of(ours, b_sf) + block_of(got, b_sf), FIRST_PERM)
    in_k = send(block_of(ours, b_sk) + block_of(got, b_sk), FIRST_PERM)
    in_2 = send(block_of(ours, b_kf) + block_of(got, b_kf) + in_f, SECOND_PERM)
    return block_of(ours, b_kk) + block_of(got, b_kk) + in_k + in_2


def gather_blocks(fin, where):
    core, key1, key2 = where
    a = send(fin, SECOND_PERM)
    b = send(fin, FIRST_PERM)
    c = send(a, FIRST_PERM)
    out = jnp.zeros((8 * BLK, fin.shape[1]), fin.dtype)
    mine = [(fin, key1 * 2 + key2), (a, key1 * 2 + 1 - key2), (b, (1 - key1) * 2 + key2), (c, (1 - key1) * 2 + 1 - key2)]
    other = [(fin, key2 * 2 + key1), (a, key2 * 2 + 1 - key1), (b, (1 - key2) * 2 + key1), (c, (1 - key2) * 2 + 1 - key1)]
    for (blk, idx), (_, oidx) in zip(mine, other):
        far = send(blk, CORE_PERM)
        out = lax.dynamic_update_slice_in_dim(out, blk, (core * 4 + idx) * BLK, axis=0)
        out = lax.dynamic_update_slice_in_dim(out, far, ((1 - core) * 4 + oidx) * BLK, axis=0)
    return out


def dot_rows(lhs, rhs):
    return lax.dot_general(lhs, rhs, (((0,), (0,)), ((), ())), preferred_element_type=jnp.float32)


def weight_grad(lhs, rhs, where):
    core = where[0]
    theirs = dot_rows(lax.dynamic_slice_in_dim(lhs, (1 - core) * 1024, 1024, axis=1), rhs)
    ours = dot_rows(lax.dynamic_slice_in_dim(lhs, core * 1024, 1024, axis=1), rhs)
    return reduce_block(theirs, ours, where)


def stats(pre_act):
    return jnp.stack([jnp.sum(pre_act, axis=1), jnp.sum(pre_act * pre_act, axis=1)])


def batch_norm(pre_act, num_rows, cid):
    totals = sum_devices(stats(pre_act).reshape(4, -1), cid).reshape(2, 2, -1) / num_rows
    inv_std = lax.rsqrt(totals[1] - totals[0] * totals[0] + BN_EPS)[:, None, :]
    return (pre_act - totals[0][:, None, :]) * inv_std, inv_std


def run_layer(hidden, weight, gain_vec, shift_vec, num_rows, cid):
    pre_act = jnp.einsum('vnf,fd->vnd', hidden, weight, preferred_element_type=jnp.float32)
    normed, inv_std = batch_norm(pre_act, num_rows, cid)
    post_affine = gain_vec * normed + shift_vec
    return jnp.maximum(post_affine, 0.0).astype(jnp.bfloat16), post_affine, normed, inv_std


def affine_backward(grad_hid, post_affine, normed, inv_std, gain_vec, num_rows, cid):
    grad_act = jnp.where(post_affine > 0, grad_hid, 0.0)
    local_sums = jnp.stack([jnp.sum(grad_act * normed, axis=1), jnp.sum(grad_act, axis=1)])
    totals = sum_devices(local_sums.reshape(4, -1), cid).reshape(2, 2, -1)
    grad_pre = (gain_vec * inv_std) * (grad_act - totals[1][:, None, :] / num_rows - normed * (totals[0][:, None, :] / num_rows))
    return grad_pre.astype(jnp.bfloat16), jnp.sum(totals[0], axis=0), jnp.sum(totals[1], axis=0)


def device_step(feat_a, feat_b, w_first, w_second, w_third, gain_first, shift_first, gain_second, shift_second, lam_off):
    num_rows = feat_a.shape[0] * NDEV
    where = place()
    core, key1, key2 = where
    both_views = jnp.stack([feat_a, feat_b])
    hid_one, post_one, norm_one, inv_one = run_layer(both_views, w_first, gain_first, shift_first, num_rows, 0)
    hid_two, post_two, norm_two, inv_two = run_layer(hid_one, w_second, gain_second, shift_second, num_rows, 1)
    proj_out = jnp.einsum('vnf,fd->vnd', hid_two, w_third, preferred_element_type=jnp.float32)
    emb_norm, inv_three = batch_norm(proj_out, num_rows, 2)
    emb_bf = emb_norm.astype(jnp.bfloat16)
    corr_blk = weight_grad(emb_bf[0], emb_bf[1], where) / num_rows
    first_row = (core * 4 + key1 * 2 + key2) * BLK
    diag_mask = lax.broadcasted_iota(jnp.int32, corr_blk.shape, 0) + first_row == lax.broadcasted_iota(jnp.int32, corr_blk.shape, 1)
    loss_part = jnp.sum(jnp.where(diag_mask, (1.0 - corr_blk) ** 2, lam_off * (corr_blk * corr_blk)))
    grad_blk = jnp.where(diag_mask, -2.0 * (1.0 - corr_blk), 2.0 * lam_off * corr_blk).astype(jnp.bfloat16)
    grad_corr = gather_blocks(grad_blk, where)
    grad_emb_a = lax.dot_general(emb_bf[1], grad_corr, (((1,), (1,)), ((), ())), preferred_element_type=jnp.float32)
    grad_emb_b = jnp.dot(emb_bf[0], grad_corr, preferred_element_type=jnp.float32)
    grad_emb = jnp.stack([grad_emb_a, grad_emb_b]) / num_rows
    local_sums = jnp.stack([jnp.sum(grad_emb, axis=1), jnp.sum(grad_emb * emb_norm, axis=1)]).reshape(4, -1)
    loss_row = jnp.full((1, local_sums.shape[1]), loss_part, jnp.float32)
    totals = sum_devices(jnp.concatenate([local_sums, loss_row, jnp.zeros((3, local_sums.shape[1]), jnp.float32)]), 3)
    total_loss = totals[4, 0]
    totals = totals[:4].reshape(2, 2, -1) / num_rows
    grad_proj = (inv_three * (grad_emb - totals[0][:, None, :] - emb_norm * totals[1][:, None, :])).astype(jnp.bfloat16)
    flat = lambda t: t.reshape(-1, t.shape[-1])
    third_blk = weight_grad(flat(hid_two), flat(grad_proj), where)
    grad_hid_two = jnp.einsum('wof,ef->woe', grad_proj, w_third, preferred_element_type=jnp.float32)
    grad_pre_two, grad_gain_second, grad_shift_second = affine_backward(grad_hid_two, post_two, norm_two, inv_two, gain_second, num_rows, 4)
    second_blk = weight_grad(flat(hid_one), flat(grad_pre_two), where)
    grad_hid_one = jnp.einsum('wof,ef->woe', grad_pre_two, w_second, preferred_element_type=jnp.float32)
    grad_pre_one, grad_gain_first, grad_shift_first = affine_backward(grad_hid_one, post_one, norm_one, inv_one, gain_first, num_rows, 5)
    first_blk = weight_grad(flat(both_views), flat(grad_pre_one), where)
    grad_third = gather_blocks(third_blk, where)
    grad_second = gather_blocks(second_blk, where)
    grad_first = gather_blocks(first_blk, where)
    return (total_loss, grad_first, grad_second, grad_third, grad_gain_first, grad_shift_first, grad_gain_second, grad_shift_second)


def solution(mesh):
    row_spec = P(ROW_AXES, None)
    repl_spec = P()
    return jax.shard_map(device_step, mesh=mesh, in_specs=(row_spec, row_spec) + (repl_spec,) * 8, out_specs=(repl_spec,) * 8, check_vma=False)
```
